32 devices in a mesh: blk: 4 (over y, x), tok: 8 (over z, core).
Axes of the slice: x: 2, y: 2, z: 4, core: 2. Of those that a mesh axis runs over, the one named last changes fastest.
Arguments:
- states: bfloat16 [256, 3584], P('tok'), may hold values from -30 to 30
- head: bfloat16 [3584, 32768], P(None, ('blk', 'tok')), may hold values from -0.2 to 0.2
- targets: int32 [256], P('tok'), may hold values from 0 to 32767
- ref_loss: float32 [256], P('tok'), may hold values from 0 to 8
- seq_ids: int32 [256], P('tok'), may hold values from 0 to 127, never falling along the last dimension, each value on 1 to 4 neighbouring positions
Outputs:
- excess: float32 [256], P('tok')
- seq_score: float32 [128], replicated
The draws below stay inside these ranges and needn't reach their ends.
Inputs may be any that keep to these rules, and one draw needn't show every extreme that they name: `seq_ids`: sequence numbers never fall along the tokens; every number from 0 to 127 occurs, on 1 to 4 consecutive tokens.
All inputs are finite; a program needn't handle non-finite values.
Results may differ from the reference program's by a relative error of at most 0.0003.
Values may be sent and summed in bfloat16 or wider, within the bound.
A program may use at most 64 MiB of HBM per device.

```python
import math
import jax
import jax.numpy as jnp
import numpy as np
from jax import lax

D = 3584
VOCAB = 32768
TOKENS = 256
SEQS = 128


def joint_draw(key):
    keys = jax.random.split(jax.random.fold_in(key, 7), 4)
    col_scale = jnp.exp(jax.random.uniform(keys[1], (VOCAB,), jnp.float32, math.log(0.5), math.log(2.0)))
    head = jax.random.normal(keys[0], (D, VOCAB), jnp.float32) / math.sqrt(D) * col_scale[None, :]
    head = jnp.clip(head, -0.19921875, 0.19921875)
    base = jax.random.normal(keys[2], (TOKENS, D), jnp.float32)
    row_scale = jnp.exp(jax.random.uniform(keys[3], (TOKENS, 1), jnp.float32, 0.0, math.log(2.0)))
    states = 3.0 * base * row_scale
    states = jnp.clip(states, -30.0, 30.0)
    return (states, head)


def draw_states(key, part):
    return joint_draw(key)[0].astype(jnp.bfloat16)


def draw_head(key, part):
    return joint_draw(key)[1].astype(jnp.bfloat16)


def plant(array, key, smallest, largest):
    spot = [jax.random.randint(jax.random.fold_in(key, axis), (), 0, length) for axis, length in enumerate(array.shape)]
    longest = array.shape.index(max(array.shape))
    neighbour = spot[:longest] + [(spot[longest] + 1) % array.shape[longest]] + spot[longest + 1:]
    return array.at[tuple(spot)].set(smallest).at[tuple(neighbour)].set(largest)


def block_levels(stream_key, extent, cuts, least, largest):
    loudness, own = 1.0, jax.random.fold_in(stream_key, 6)
    for axis_at, parts in cuts:
        draws = jnp.exp(jax.random.uniform(jax.random.fold_in(own, axis_at), (parts,), jnp.float32, least / len(cuts), largest / len(cuts)))
        loudness = loudness * jnp.repeat(draws, extent[axis_at] // parts).reshape([-1 if axis == axis_at else 1 for axis in range(len(extent))])
    return loudness


def split_up(count, total, most, lean):
    portions = [(1 << 20) // math.isqrt(rank ** lean) + 1 for rank in range(2, count + 1)]
    spare, holding = total - most - (count - 1), [1] * (count - 1)
    while spare > 0:
        free = [i for i in range(count - 1) if holding[i] < most]
        mass, remaining = sum([portions[i] for i in free]), spare
        for i in free:
            extra = min(most - holding[i], max(1, remaining * portions[i] // mass), spare)
            holding[i] = holding[i] + extra
            spare = spare - extra
    return np.array([most] + holding)


def ragged(key, count, total, reach, slope):
    if count == 2:
        one = jax.random.randint(key, (), max(1, total - reach), min(reach, total - 1) + 1)
        return jnp.stack([one, total - one])
    lengths = jnp.asarray(split_up(count, total, reach, slope), jnp.int32)
    pairs = (count - 1) // 2
    source_of, sink = lengths[1:1 + 2 * pairs:2], lengths[2:2 + 2 * pairs:2]
    margin = jnp.minimum(source_of - 1, reach - sink)
    shifted = jax.random.randint(jax.random.fold_in(key, 1), (pairs,), 0, 1 << 20) % (margin + 1)
    lengths = lengths.at[1:1 + 2 * pairs:2].set(source_of - shifted).at[2:2 + 2 * pairs:2].set(sink + shifted)
    return lengths[jax.random.permutation(jax.random.fold_in(key, 2), count)]


def setup_inputs(seed: int = 0) -> dict:
    key_of = jax.random.split(jax.random.key(seed), 6)
    return {
        "states": draw_states(jax.random.fold_in(key_of[5], 71), 0),
        "head": draw_head(jax.random.fold_in(key_of[5], 71), 0),
        "targets": plant(jax.random.randint(key_of[2], (TOKENS,), 0, VOCAB), jax.random.fold_in(key_of[2], 1), 0, VOCAB - 1).astype(jnp.int32),
        "ref_loss": jnp.clip(8.0 * jax.random.uniform(key_of[3], (TOKENS,), jnp.float32) ** block_levels(key_of[3], (TOKENS,), ((0, 8),), -0.2, 0.2), 0.0, 8.0),
        "seq_ids": jnp.searchsorted(jnp.cumsum(ragged(key_of[4], SEQS, TOKENS, 4, 2)), jnp.arange(TOKENS), side="right").astype(jnp.int32),
    }


def reference(states, head, targets, ref_loss, seq_ids):
    group = min(256, TOKENS)
    while TOKENS % group != 0:
        group = group // 2
    blocks = TOKENS // group

    def score(operands):
        token_rows, target_ids = operands
        logits = jnp.dot(token_rows, head, preferred_element_type=jnp.float32)
        highest = jnp.max(logits, axis=1)
        log_total = highest + jnp.log(jnp.sum(jnp.exp(logits - highest[:, None]), axis=1))
        picked = jnp.take_along_axis(logits, target_ids[:, None].astype(jnp.int32), axis=1)[:, 0]
        return log_total - picked

    values = lax.map(score, (states.reshape(blocks, group, D), targets.reshape(blocks, group)))
    excess = values.reshape(TOKENS) - ref_loss
    totals = jax.ops.segment_sum(excess, seq_ids, num_segments=SEQS)
    counts = jax.ops.segment_sum(jnp.ones((TOKENS,), jnp.float32), seq_ids, num_segments=SEQS)
    return excess, totals / counts
```

```python
import functools

import jax
import jax.numpy as jnp
from jax import lax
from jax.experimental import pallas as pl
from jax.experimental.pallas import tpu as pltpu
from jax.sharding import PartitionSpec as P

quarters = 4
lanes = 128


def flipped(index, bits):
    bit = 1
    result = index
    while bit <= bits:
        if bits & bit:
            result = result + bit - 2 * bit * lax.rem(lax.div(index, bit), 2)
        bit = 2 * bit
    return result


def kernel(
    blks, toks, states, head, targets, ref_loss, seq_ids, excess_out, score_out,
    rows, weights, logits, meta, columns, stats,
    states_sem, head_sem, send_sem, z_sem, side_sem, half_sem, core_sem, own_sem,
    meta_send, meta_recv, stats_send, stats_recv,
):
    blk, tok = lax.axis_index("blk"), lax.axis_index("tok")
    local = states.shape[0]
    depth = weights.shape[1]
    width = weights.shape[2]
    tokens = toks * local
    seqs = score_out.shape[1]
    chips = toks // 2
    devices = blks * toks
    me = blk * toks + tok
    mine = lax.rem(blk, quarters)
    partner = flipped(tok, 1)

    def place(owner, begin=0, size=local):
        return pl.ds(pl.multiple_of(owner * local + begin, 16), size)

    def send(source, target, sent, received, to_blk, to_tok):
        pltpu.make_async_remote_copy(
            src_ref=source, dst_ref=target, send_sem=sent, recv_sem=received,
            device_id={"blk": to_blk, "tok": to_tok},
            device_id_type=pl.DeviceIdType.MESH,
        ).start()

    def pass_on(part, received, to_blk, to_tok):
        send(part, part, send_sem, received, to_blk, to_tok)

    def arrived(part, received):
        pltpu.make_async_copy(part, part, received).wait()

    states_in = []
    for step in range(quarters):
        part = flipped(mine, step)
        states_in.append(pltpu.make_async_copy(
            states.at[:, pl.ds(pl.multiple_of(part * depth, lanes), depth)],
            rows.at[part, place(tok)], states_sem.at[step]))
        states_in[-1].start()
    head_in = []
    for step in range(quarters):
        part = flipped(mine, step)
        head_in.append(pltpu.make_async_copy(
            head.at[pl.ds(pl.multiple_of(part * depth, 16), depth)],
            weights.at[part], head_sem.at[step]))
        head_in[-1].start()

    barrier = pltpu.get_barrier_semaphore()
    greeted = [(blk, flipped(tok, step)) for step in range(1, toks)]
    greeted += [(flipped(blk, 1), tok), (flipped(blk, 2), tok)]
    for to_blk, to_tok in greeted:
        pl.semaphore_signal(
            barrier, inc=1, device_id={"blk": to_blk, "tok": to_tok},
            device_id_type=pl.DeviceIdType.MESH)
    meta[tok] = jnp.zeros((8, lanes), jnp.float32)
    meta[tok, 0:1, 0:local] = targets[...].astype(jnp.float32)
    meta[tok, 1:2, 0:local] = ref_loss[...]
    meta[tok, 2:3, 0:local] = seq_ids[...].astype(jnp.float32)
    states_in[0].wait()
    pl.semaphore_wait(barrier, len(greeted))

    for step in range(1, chips):
        pass_on(rows.at[mine, place(tok)], z_sem.at[step], blk, flipped(tok, 2 * step))
    for step in range(1, toks):
        send(meta.at[tok], meta.at[tok], meta_send, meta_recv, blk, flipped(tok, step))
    for step in range(1, quarters):
        states_in[step].wait()
    pass_on(rows.at[:, place(tok)], own_sem.at[0], blk, partner)

    def piece(part, step, begin=0, size=local, core=0):
        return rows.at[flipped(mine, part), place(flipped(tok, 2 * step + core), begin, size)]

    half = local // 2

    def forward_z(step):
        arrived(piece(0, step), z_sem.at[step])
        pass_on(piece(0, step), side_sem.at[0, step], flipped(blk, 1), tok)
        pass_on(piece(0, step), side_sem.at[1, step], flipped(blk, 2), tok)
        pass_on(piece(0, step), core_sem.at[0, step], blk, partner)

    def forward_sides(step):
        for side in (0, 1):
            part = side + 1
            arrived(piece(part, step), side_sem.at[side, step])
            pass_on(piece(part, step, side * half, half), half_sem.at[side, step],
                    flipped(blk, 3 - part), tok)
            pass_on(piece(part, step), core_sem.at[part, step], blk, partner)

    def forward_halves(step):
        for side in (0, 1):
            arrived(piece(3, step, side * half, half), half_sem.at[side, step])
            pass_on(piece(3, step, side * half, half), core_sem.at[3 + side, step], blk, partner)

    def multiply(part):
        for step in range(1, chips):
            if part < 3:
                arrived(piece(part, step, core=1), core_sem.at[part, step])
            else:
                for side in (0, 1):
                    arrived(piece(part, step, side * half, half, core=1),
                            core_sem.at[3 + side, step])
        head_in[part].wait()
        at = flipped(mine, part)
        block = min(tokens, 256)

        def one(index):
            here = pl.ds(pl.multiple_of(index * block, block), block)
            product = jnp.dot(rows[at, here], weights[at], preferred_element_type=jnp.float32)
            logits[here] = product if part == 0 else logits[here] + product

        if block == tokens:
            one(0)
        else:
            pl.loop(0, tokens // block)(one)

    jobs = []
    for step in range(1, chips):
        jobs.append((3 * step, forward_z, step))
        jobs.append((3 * step + 4, forward_sides, step))
        jobs.append((3 * step + 8, forward_halves, step))
    last = 3 * (chips - 1)
    jobs = sorted(jobs, key=lambda job: job[0])
    multiplied = 0
    for when, job, step in jobs:
        if when > last + 4 and multiplied == 0:
            arrived(rows.at[:, place(partner)], own_sem.at[0])
            arrived(meta.at[pl.ds(0, toks - 1)], meta_recv)
            multiply(0)
            multiplied = 1
        job(step)
    for part in range(multiplied, quarters):
        if part == 0:
            arrived(rows.at[:, place(partner)], own_sem.at[0])
            arrived(meta.at[pl.ds(0, toks - 1)], meta_recv)
        if part == 3:
            for owner in range(toks):
                columns[owner * local:(owner + 1) * local] = meta[owner].T[0:local]
        multiply(part)

    block = min(tokens, 256)
    for begin in range(0, tokens, block):
        here = pl.ds(begin, block)
        values = logits[here]
        highest = jnp.max(values, axis=1, keepdims=True)
        scaled = jnp.sum(jnp.exp(values - highest), axis=1, keepdims=True)
        total = highest + jnp.log(scaled)
        spots = lax.broadcasted_iota(jnp.int32, values.shape, 1) + me * width
        wanted = columns[here, 0:1].astype(jnp.int32)
        picked = jnp.sum(jnp.where(spots == wanted, values, 0.0), axis=1, keepdims=True)
        lane = lax.broadcasted_iota(jnp.int32, (block, lanes), 1)
        packed = jnp.where(lane == 0, total, jnp.where(lane == 1, picked, columns[here, 1:2]))
        turned = packed.T
        stats[devices - 1, :, here] = turned[0:2]
        logits[0:1, here] = turned[2:3]

    def broadcast(by, _):
        to = lax.rem(me + by, devices)
        send(stats.at[devices - 1], stats.at[by - 1], stats_send, stats_recv,
             lax.div(to, toks), lax.rem(to, toks))
        return _

    lax.fori_loop(1, devices, broadcast, 0)

    member = (columns[:, 2:3].astype(jnp.int32)
              == lax.broadcasted_iota(jnp.int32, (tokens, seqs), 1)).astype(jnp.float32)
    own = lax.broadcasted_iota(jnp.int32, (tokens, lanes), 1)
    own = (lax.broadcasted_iota(jnp.int32, (tokens, lanes), 0) == own + tok * local)
    chosen = jnp.concatenate([member, own.astype(jnp.float32)], axis=1)
    loss = logits[0:1, 0:tokens]

    arrived(stats.at[pl.ds(0, devices - 1)], stats_recv)
    gathered = stats[...]
    peak = jnp.max(gathered, axis=0)
    total = peak + jnp.log(jnp.sum(jnp.exp(gathered - peak[None]), axis=0))
    picked = jnp.sum(gathered, axis=0)
    excess = total[0:1] - picked[1:2] - loss
    left = jnp.where(lax.broadcasted_iota(jnp.int32, (8, tokens), 0) == 0, excess, 1.0)
    sums = jnp.dot(left, chosen, precision=lax.Precision.HIGHEST,
                   preferred_element_type=jnp.float32)
    excess_out[...] = sums[0:1, seqs:seqs + local]
    score_out[...] = sums[0:1, 0:seqs] / sums[1:2, 0:seqs]

    arrived(rows.at[:, pl.ds(0, tokens - local)], send_sem)
    arrived(meta.at[pl.ds(0, toks - 1)], meta_send)
    arrived(stats.at[pl.ds(0, devices - 1)], stats_send)


def on_device(states, head, targets, ref_loss, seq_ids):
    blks, toks = lax.axis_size("blk"), lax.axis_size("tok")
    local, model = states.shape
    width = head.shape[1]
    tokens = local * toks
    seqs = tokens // 2
    devices = blks * toks
    depth = model // quarters
    chips = toks // 2
    dma = pltpu.SemaphoreType.DMA
    small = pl.BlockSpec(memory_space=pltpu.VMEM)
    large = pl.BlockSpec(memory_space=pl.ANY)
    excess, score = pl.pallas_call(
        functools.partial(kernel, blks, toks),
        out_shape=(
            jax.ShapeDtypeStruct((1, local), jnp.float32),
            jax.ShapeDtypeStruct((1, seqs), jnp.float32),
        ),
        in_specs=[large, large, small, small, small],
        out_specs=(small, small),
        scratch_shapes=[
            pltpu.VMEM((quarters, tokens, depth), jnp.bfloat16),
            pltpu.VMEM((quarters, depth, width), jnp.bfloat16),
            pltpu.VMEM((tokens, width), jnp.float32),
            pltpu.VMEM((toks, 8, lanes), jnp.float32),
            pltpu.VMEM((tokens, 8), jnp.float32),
            pltpu.VMEM((devices, 2, tokens), jnp.float32),
            dma((quarters,)),
            dma((quarters,)),
            dma,
            dma((chips,)),
            dma((2, chips)),
            dma((2, chips)),
            dma((5, chips)),
            dma((1,)),
            dma, dma, dma, dma,
        ],
        compiler_params=pltpu.CompilerParams(collective_id=0, has_side_effects=True),
    )(states, head, targets.reshape(1, local), ref_loss.reshape(1, local),
      seq_ids.reshape(1, local))
    return excess.reshape(local), score.reshape(seqs)


def solution(mesh):
    placed = (P("tok", None), P(None, ("blk", "tok")), P("tok"), P("tok"), P("tok"))
    return jax.shard_map(
        on_device, mesh=mesh, in_specs=placed, out_specs=(P("tok"), P()), check_vma=False
    )
```

```python
import functools

import jax
import jax.numpy as jnp
from jax import lax
from jax.experimental import pallas as pl
from jax.experimental.pallas import tpu as pltpu
from jax.sharding import PartitionSpec as P

quarters = 4
lanes = 128


def flipped(index, bits):
    bit = 1
    result = index
    while bit <= bits:
        if bits & bit:
            result = result + bit - 2 * bit * lax.rem(lax.div(index, bit), 2)
        bit = 2 * bit
    return result


def kernel(
    blks, toks, states, head, targets, ref_loss, seq_ids, excess_out, score_out,
    rows, weights, logits, meta, columns, stats,
    small_ints, small_floats, states_sem, head_sem, small_sem, send_sem, z_sem, side_sem, half_sem, core_sem, own_sem,
    meta_send, meta_recv, stats_send, stats_recv,
):
    blk, tok = lax.axis_index("blk"), lax.axis_index("tok")
    local = states.shape[0]
    depth = weights.shape[1]
    width = weights.shape[2]
    tokens = toks * local
    seqs = score_out.shape[1]
    chips = toks // 2
    devices = blks * toks
    me = blk * toks + tok
    mine = lax.rem(blk, quarters)
    partner = flipped(tok, 1)

    def place(owner, begin=0, size=local):
        return pl.ds(pl.multiple_of(owner * local + begin, 16), size)

    def send(source, target, sent, received, to_blk, to_tok):
        pltpu.make_async_remote_copy(
            src_ref=source, dst_ref=target, send_sem=sent, recv_sem=received,
            device_id={"blk": to_blk, "tok": to_tok},
            device_id_type=pl.DeviceIdType.MESH,
        ).start()

    def pass_on(part, received, to_blk, to_tok):
        send(part, part, send_sem, received, to_blk, to_tok)

    def arrived(part, received):
        pltpu.make_async_copy(part, part, received).wait()

    states_in = []
    for step in range(quarters):
        part = flipped(mine, step)
        states_in.append(pltpu.make_async_copy(
            states.at[:, pl.ds(pl.multiple_of(part * depth, lanes), depth)],
            rows.at[part, place(tok)], states_sem.at[step]))
        states_in[-1].start()
    small_in = [
        pltpu.make_async_copy(targets, small_ints.at[0], small_sem.at[0]),
        pltpu.make_async_copy(ref_loss, small_floats, small_sem.at[1]),
        pltpu.make_async_copy(seq_ids, small_ints.at[1], small_sem.at[2]),
    ]
    for copy in small_in:
        copy.start()
    head_in = []
    for step in range(quarters):
        part = flipped(mine, step)
        head_in.append(pltpu.make_async_copy(
            head.at[pl.ds(pl.multiple_of(part * depth, 16), depth)],
            weights.at[part], head_sem.at[step]))
        head_in[-1].start()

    barrier = pltpu.get_barrier_semaphore()
    greeted = [(blk, flipped(tok, step)) for step in range(1, toks)]
    greeted += [(flipped(blk, 1), tok), (flipped(blk, 2), tok)]
    for to_blk, to_tok in greeted:
        pl.semaphore_signal(
            barrier, inc=1, device_id={"blk": to_blk, "tok": to_tok},
            device_id_type=pl.DeviceIdType.MESH)
    states_in[0].wait()
    pl.semaphore_wait(barrier, len(greeted))

    half = local // 2
    for step in range(1, chips):
        for cut in (0, 1):
            pass_on(rows.at[mine, place(tok, cut * half, half)], z_sem.at[step, cut], blk,
                    flipped(tok, 2 * step))
    for copy in small_in:
        copy.wait()
    meta[tok] = jnp.zeros((8, lanes), jnp.float32)
    meta[tok, 0:1, 0:local] = small_ints[0].astype(jnp.float32)
    meta[tok, 1:2, 0:local] = small_floats[...]
    meta[tok, 2:3, 0:local] = small_ints[1].astype(jnp.float32)
    for step in range(1, quarters):
        states_in[step].wait()
    for cut in (0, 1):
        pass_on(rows.at[flipped(mine, 3), place(tok, cut * half, half)], half_sem.at[1, cut],
                blk, flipped(tok, 2))
    pass_on(rows.at[:, place(tok)], own_sem.at[0], blk, partner)

    for step in range(1, toks):
        send(meta.at[tok], meta.at[tok], meta_send, meta_recv, blk, flipped(tok, step))

    def piece(part, step, begin=0, size=local, core=0):
        return rows.at[flipped(mine, part), place(flipped(tok, 2 * step + core), begin, size)]

    def forward_z(step, cut):
        here = piece(0, step, cut * half, half)
        arrived(here, z_sem.at[step, cut])
        pass_on(here, side_sem.at[0, step, cut], flipped(blk, 1), tok)
        pass_on(here, side_sem.at[1, step, cut], flipped(blk, 2), tok)
        pass_on(here, core_sem.at[0, step, cut], blk, partner)

    def forward_sides(step, cut):
        for side in (cut, 1 - cut):
            part = side + 1
            here = piece(part, step, cut * half, half)
            arrived(here, side_sem.at[side, step, cut])
            if side == cut and step > 1:
                pass_on(here, half_sem.at[step, cut], flipped(blk, 3 - part), tok)
            pass_on(here, core_sem.at[part, step, cut], blk, partner)

    def forward_halves(step, cut):
        here = piece(3, step, cut * half, half)
        arrived(here, half_sem.at[step, cut])
        pass_on(here, core_sem.at[3, step, cut], blk, partner)

    def multiply(part):
        for step in range(1, chips):
            for cut in (0, 1):
                arrived(piece(part, step, cut * half, half, core=1),
                        core_sem.at[part, step, cut])
        head_in[part].wait()
        at = flipped(mine, part)
        block = min(tokens, 256)

        def one(index):
            here = pl.ds(pl.multiple_of(index * block, block), block)
            product = jnp.dot(rows[at, here], weights[at], preferred_element_type=jnp.float32)
            logits[here] = product if part == 0 else logits[here] + product

        if block == tokens:
            one(0)
        else:
            pl.loop(0, tokens // block)(one)

    jobs = []
    for order in range(2 * (chips - 1)):
        spot = (1 + order // 2, order % 2)
        jobs.append((7 * order, forward_z, spot))
        jobs.append((7 * order + 23, forward_sides, spot))
        jobs.append((7 * order + 45, forward_halves, spot))
    jobs = sorted(jobs, key=lambda job: job[0])
    last = 7 * (2 * chips - 3)
    cuts = [last + 23, last + 31, last + 38, last + 45]
    low = -1
    for part in range(quarters):
        for when, job, spot in jobs:
            if low < when <= cuts[part]:
                job(*spot)
        low = cuts[part]
        if part == 0:
            arrived(rows.at[:, place(partner)], own_sem.at[0])
            arrived(meta.at[pl.ds(0, toks - 1)], meta_recv)
            for owner in range(toks):
                columns[owner * local:(owner + 1) * local] = meta[owner].T[0:local]
        multiply(part)

    block = min(tokens, 256)
    for begin in range(0, tokens, block):
        here = pl.ds(begin, block)
        values = logits[here]
        highest = jnp.max(values, axis=1, keepdims=True)
        scaled = jnp.sum(jnp.exp(values - highest), axis=1, keepdims=True)
        total = highest + jnp.log(scaled)
        spots = lax.broadcasted_iota(jnp.int32, values.shape, 1) + me * width
        wanted = columns[here, 0:1].astype(jnp.int32)
        picked = jnp.sum(jnp.where(spots == wanted, values, 0.0), axis=1, keepdims=True)
        lane = lax.broadcasted_iota(jnp.int32, (block, lanes), 1)
        packed = jnp.where(lane == 0, total, jnp.where(lane == 1, picked, columns[here, 1:2]))
        turned = packed.T
        stats[devices - 1, :, here] = turned[0:2]
        logits[0:1, here] = turned[2:3]

    def broadcast(by, _):
        to = lax.rem(me + by, devices)
        send(stats.at[devices - 1], stats.at[by - 1], stats_send, stats_recv,
             lax.div(to, toks), lax.rem(to, toks))
        return _

    lax.fori_loop(1, devices, broadcast, 0)

    member = (columns[:, 2:3].astype(jnp.int32)
              == lax.broadcasted_iota(jnp.int32, (tokens, seqs), 1)).astype(jnp.float32)
    own = lax.broadcasted_iota(jnp.int32, (tokens, lanes), 1)
    own = (lax.broadcasted_iota(jnp.int32, (tokens, lanes), 0) == own + tok * local)
    chosen = jnp.concatenate([member, own.astype(jnp.float32)], axis=1)
    loss = logits[0:1, 0:tokens]

    arrived(stats.at[pl.ds(0, devices - 1)], stats_recv)
    gathered = stats[...]
    peak = jnp.max(gathered, axis=0)
    total = peak + jnp.log(jnp.sum(jnp.exp(gathered - peak[None]), axis=0))
    picked = jnp.sum(gathered, axis=0)
    excess = total[0:1] - picked[1:2] - loss
    left = jnp.where(lax.broadcasted_iota(jnp.int32, (8, tokens), 0) == 0, excess, 1.0)
    sums = jnp.dot(left, chosen, precision=lax.Precision.HIGHEST,
                   preferred_element_type=jnp.float32)
    excess_out[...] = sums[0:1, seqs:seqs + local]
    score_out[...] = sums[0:1, 0:seqs] / sums[1:2, 0:seqs]

    arrived(rows.at[:, pl.ds(0, tokens - local)], send_sem)
    arrived(meta.at[pl.ds(0, toks - 1)], meta_send)
    arrived(stats.at[pl.ds(0, devices - 1)], stats_send)


def on_device(states, head, targets, ref_loss, seq_ids):
    blks, toks = lax.axis_size("blk"), lax.axis_size("tok")
    local, model = states.shape
    width = head.shape[1]
    tokens = local * toks
    seqs = tokens // 2
    devices = blks * toks
    depth = model // quarters
    chips = toks // 2
    dma = pltpu.SemaphoreType.DMA
    small = pl.BlockSpec(memory_space=pltpu.VMEM)
    large = pl.BlockSpec(memory_space=pl.ANY)
    excess, score = pl.pallas_call(
        functools.partial(kernel, blks, toks),
        out_shape=(
            pltpu.VMEM((1, local), jnp.float32),
            pltpu.VMEM((1, seqs), jnp.float32),
        ),
        in_specs=[large] * 5,
        out_specs=(small, small),
        scratch_shapes=[
            pltpu.VMEM((quarters, tokens, depth), jnp.bfloat16),
            pltpu.VMEM((quarters, depth, width), jnp.bfloat16),
            pltpu.VMEM((tokens, width), jnp.float32),
            pltpu.VMEM((toks, 8, lanes), jnp.float32),
            pltpu.VMEM((tokens, 8), jnp.float32),
            pltpu.VMEM((devices, 2, tokens), jnp.float32),
            pltpu.VMEM((2, 1, local), jnp.int32),
            pltpu.VMEM((1, local), jnp.float32),
            dma((quarters,)),
            dma((quarters,)),
            dma((3,)),
            dma,
            dma((chips, 2)),
            dma((2, chips, 2)),
            dma((chips, 2)),
            dma((4, chips, 2)),
            dma((1,)),
            dma, dma, dma, dma,
        ],
        compiler_params=pltpu.CompilerParams(collective_id=0, has_side_effects=True),
    )(states, head, targets.reshape(1, local), ref_loss.reshape(1, local),
      seq_ids.reshape(1, local))
    return excess.reshape(local), score.reshape(seqs)


def solution(mesh):
    placed = (P("tok", None), P(None, ("blk", "tok")), P("tok"), P("tok"), P("tok"))
    return jax.shard_map(
        on_device, mesh=mesh, in_specs=placed, out_specs=(P("tok"), P()), check_vma=False
    )
```
